512 devices in a mesh: rows: 32 (over z, x), tp: 2 (over core), job: 8 (over y).
Axes of the slice: x: 4, y: 8, z: 8, core: 2. Of those that a mesh axis runs over, the one named last changes fastest.
Arguments:
- train_query: bfloat16 [16384, 2048], P(('job', 'rows'), 'tp'), parts along dimension 0, may hold values from -0.125 to 0.125
- low_query: bfloat16 [16384, 16], P(('job', 'rows')), parts along dimension 0, may hold values from -0.125 to 0.125
- high_query: bfloat16 [128, 2048], P('job', 'tp'), parts along dimension 0, may hold values from -1.5 to 1.5
- train_key: bfloat16 [16384, 512], P(('job', 'rows'), 'tp'), parts along dimension 0, may hold values from -0.125 to 0.125
- low_key: bfloat16 [16384, 16], P(('job', 'rows')), parts along dimension 0, may hold values from -0.125 to 0.125
- high_key: bfloat16 [128, 512], P('job', 'tp'), parts along dimension 0, may hold values from -1.5 to 1.5
- train_value: bfloat16 [16384, 512], P(('job', 'rows'), 'tp'), parts along dimension 0, may hold values from -0.125 to 0.125
- low_value: bfloat16 [16384, 16], P(('job', 'rows')), parts along dimension 0, may hold values from -0.125 to 0.125
- high_value: bfloat16 [128, 512], P('job', 'tp'), parts along dimension 0, may hold values from -1.5 to 1.5
- norm_train: float32 [16384], P(('job', 'rows', 'tp')), parts along dimension 0, may hold values from 0.25 to 1.75
- norm_step: float32 [16384], P(('job', 'rows', 'tp')), parts along dimension 0, may hold values from -0.3 to 0.3
Outputs:
- serve_query: bfloat16 [16384, 2048], P(('job', 'tp')), parts along dimension 0
- serve_key: bfloat16 [4096, 2048], P(('job', 'tp')), parts along dimension 0
- serve_value: bfloat16 [4096, 2048], P(('job', 'tp')), parts along dimension 0
- serve_norm: bfloat16 [16384], P('job'), parts along dimension 0
The draws below stay inside these ranges and needn't reach their ends.
There are 8 independent parts, one for each index of `job`. The reference program is written for one: setup_inputs(seed, part) draws one part's arguments, and reference() takes and returns one part's arrays. A program takes and returns all parts, laid end to end along the dimension named above; each array names one. Nothing has to cross between parts.
All inputs are finite; a program needn't handle non-finite values.
Results may differ from the reference program's by a relative error of at most 0.001.
Values may be sent and summed in bfloat16 or wider, within the bound.
A program may use at most 64 MiB of HBM per device.

```python
import jax
import jax.numpy as jnp

D_MODEL = 2048
Q_DIM = 2048
KV_DIM = 512
RANK = 16


def level_of(stream_key, extent, pieces, low, top_value):
    gain = 1.0
    for dim, blocks in pieces:
        heights = jax.random.uniform(jax.random.fold_in(jax.random.fold_in(stream_key, 6), dim), (blocks,), jnp.float32, low / len(pieces), top_value / len(pieces))
        gain = gain * jnp.repeat(jnp.exp(heights), extent[dim] // blocks).reshape((-1,) + (1,) * (len(extent) - 1 - dim))
    return gain


def centred(own_key, shape, spread, reach, cuts=(), kind=jnp.bfloat16):
    entries = spread * jax.random.normal(own_key, shape, jnp.float32)
    if cuts:
        entries = entries * level_of(own_key, shape, cuts, -0.22, 0.18)
    return jnp.clip(entries, -reach, reach).astype(kind)


def setup_inputs(seed: int = 0, part: int = 0) -> dict:
    key_of = jax.random.split(jax.random.key(seed), 12)
    own_keys = jax.random.split(jax.random.fold_in(key_of[11], part), 12)
    return {
        "train_query": centred(own_keys[0], (D_MODEL, Q_DIM), D_MODEL ** -0.5, 0.125, ((0, 32), (1, 2))),
        "low_query": centred(own_keys[1], (D_MODEL, RANK), D_MODEL ** -0.5, 0.125, ((0, 32),)),
        "high_query": centred(own_keys[2], (RANK, Q_DIM), RANK ** -0.5, 1.5, ((1, 2),)),
        "train_key": centred(own_keys[3], (D_MODEL, KV_DIM), D_MODEL ** -0.5, 0.125, ((0, 32), (1, 2))),
        "low_key": centred(own_keys[4], (D_MODEL, RANK), D_MODEL ** -0.5, 0.125, ((0, 32),)),
        "high_key": centred(own_keys[5], (RANK, KV_DIM), RANK ** -0.5, 1.5, ((1, 2),)),
        "train_value": centred(own_keys[6], (D_MODEL, KV_DIM), D_MODEL ** -0.5, 0.125, ((0, 32), (1, 2))),
        "low_value": centred(own_keys[7], (D_MODEL, RANK), D_MODEL ** -0.5, 0.125, ((0, 32),)),
        "high_value": centred(own_keys[8], (RANK, KV_DIM), RANK ** -0.5, 1.5, ((1, 2),)),
        "norm_train": jnp.clip(1.0 + 0.15 * jax.random.normal(own_keys[9], (D_MODEL,), jnp.float32), 0.25, 1.75),
        "norm_step": jnp.clip(jax.random.uniform(own_keys[10], (D_MODEL,), jnp.float32, -0.3, 0.3) * level_of(own_keys[10], (D_MODEL,), ((0, 64),), -0.4, 0.0), -0.3, 0.3),
    }


mix_rate = 0.5


def reference(train_query, low_query, high_query, train_key, low_key, high_key, train_value, low_value, high_value, norm_train, norm_step):
    fresh_query = train_query.astype(jnp.float32) + mix_rate * jnp.dot(low_query, high_query, preferred_element_type=jnp.float32)
    fresh_key = train_key.astype(jnp.float32) + mix_rate * jnp.dot(low_key, high_key, preferred_element_type=jnp.float32)
    fresh_value = train_value.astype(jnp.float32) + mix_rate * jnp.dot(low_value, high_value, preferred_element_type=jnp.float32)
    serve_query = fresh_query.T.astype(jnp.bfloat16)
    serve_key = fresh_key.T.astype(jnp.bfloat16)
    serve_value = fresh_value.T.astype(jnp.bfloat16)
    serve_norm = (norm_train + norm_step).astype(jnp.bfloat16)
    return serve_query, serve_key, serve_value, serve_norm
```

```python
import functools
import heapq
import itertools

import jax
import jax.numpy as jnp
from jax import lax
from jax.experimental import pallas as pl
from jax.experimental.pallas import tpu as pltpu
from jax.sharding import PartitionSpec as P

MESH = pl.DeviceIdType.MESH
mix_rate = 0.5

Z, X = 8, 4
RATE = 46650.0
HOP = 2.0
DEPTH = 2

PIECES = (("x", 640, 1), ("z", 512, 1), ("z", 384, -1))
FIRST = (1, 0, 2)


def onward(d, size, far):
    if d == 0:
        return [(1, 1), (-1, -1)]
    side = 1 if d > 0 else -1
    limit = size // 2 if side == far else size // 2 - 1
    return [(d + side, side)] if abs(d) < limit else []


def forwards(item):
    kind, dx, dz = item
    out = []
    if kind == "sum_x":
        return [("x", s, ("sum_x", n, 0)) for n, s in onward(dx, X, 1)]
    if kind == "sum_z":
        return [("z", s, ("sum_z", 0, n)) for n, s in onward(dz, Z, 1)]
    axis, _, far = PIECES[kind]
    if axis == "x":
        if dz == 0:
            out += [("x", s, (kind, n, 0)) for n, s in onward(dx, X, far)]
        out += [("z", s, (kind, dx, n)) for n, s in onward(dz, Z, 1 if dx % 2 == 0 else -1)]
    else:
        if dx == 0:
            out += [("z", s, (kind, 0, n)) for n, s in onward(dz, Z, far)]
        out += [("x", s, (kind, n, dz)) for n, s in onward(dx, X, 1 if dz % 2 == 0 else -1)]
    return out


def left_to_go(item):
    after = forwards(item)
    return 1 + max(left_to_go(n) for _, _, n in after) if after else 0


def plan():
    links = {(a, s): [] for a in "xz" for s in (1, -1)}
    given = {k: [] for k in links}
    events, tick, steps = [], itertools.count(), []
    norm_x, norm_z = 1, 1

    def cost(item):
        return (512 if isinstance(item[0], str) else PIECES[item[0]][1] * 128) / RATE

    def offer(item):
        for axis, side, there in forwards(item):
            rank = -1000 if isinstance(item[0], str) else -left_to_go(there)
            links[axis, side].append((rank, next(tick), item, there))

    def begin(k, now):
        item = given[k][0]
        heapq.heappush(events, (now + cost(item), next(tick), "done", k, item))

    def feed(now):
        for k in links:
            while links[k] and len(given[k]) < DEPTH:
                links[k].sort()
                _, _, item, there = links[k].pop(0)
                steps.append(("send", k[0], k[1], item, there))
                given[k].append(there)
                if len(given[k]) == 1:
                    begin(k, now)

    offer(("sum_x", 0, 0))
    for kind in FIRST:
        offer((kind, 0, 0))
    feed(0.0)
    while events:
        now, _, what, k, item = heapq.heappop(events)
        if what == "done":
            given[k].pop(0)
            if given[k]:
                begin(k, now)
            heapq.heappush(events, (now + HOP, next(tick), "here", k, item))
            feed(now)
            continue
        steps.append(("wait", item))
        if item[0] == "sum_x":
            norm_x += 1
            if norm_x == X:
                offer(("sum_z", 0, 0))
        elif item[0] == "sum_z":
            norm_z += 1
        offer(item)
        feed(now)
        if item[0] == "sum_z" and norm_z == Z:
            steps.append(("swap",))
    return steps


def kernel(
    steps, places, tq, lq, hq, tk, lk, hk, tv, lv, hv, nt, ns, oq, ok, ov, on, *scratch
):
    vin, blocks, sums = scratch[:11], scratch[11 : 11 + len(PIECES)], scratch[11 + len(PIECES)]
    in_sem, send_sem, recv_sem, swap_sem = scratch[12 + len(PIECES) :]
    me, tp = lax.axis_index("rows"), lax.axis_index("tp")
    mz, mx = me // X, me % X

    def row(dx, dz):
        return ((mz - dz + Z) % Z) * X + (mx - dx + X) % X

    loads = [
        pltpu.make_async_copy(a, b, in_sem.at[i])
        for i, (a, b) in enumerate(zip((tq, lq, hq, tk, lk, hk, tv, lv, hv, nt, ns), vin))
    ]
    for load in loads:
        load.start()

    barrier = pltpu.get_barrier_semaphore()
    for there in (row(1, 0), row(-1, 0), row(0, 1), row(0, -1)):
        pl.semaphore_signal(barrier, inc=1, device_id={"rows": there}, device_id_type=MESH)
    pl.semaphore_signal(barrier, inc=1, device_id={"tp": 1 - tp}, device_id_type=MESH)

    for load in loads:
        load.wait()
    vtq, vlq, vhq, vtk, vlk, vhk, vtv, vlv, vhv, vnt, vns = vin

    def merged(train, low, high, lo, hi):
        product = lax.dot_general(
            low[...], high[:, lo:hi], (((0,), (0,)), ((), ())), preferred_element_type=jnp.float32
        )
        return (train[:, lo:hi].astype(jnp.float32) + mix_rate * product).astype(jnp.bfloat16)

    cut = PIECES[0][1]
    width = vtq.shape[1]
    kv = vtk.shape[1]
    sums[tp, me] = jnp.concatenate(
        [vnt[...] + vns[...], jnp.zeros((1, 128 - vnt.shape[1]), jnp.float32)], axis=1
    )
    blocks[1][me, :, :kv] = merged(vtk, vlk, vhk, 0, kv)
    blocks[1][me, :, kv:] = merged(vtv, vlv, vhv, 0, kv)
    blocks[0][me] = merged(vtq, vlq, vhq, 0, cut)
    blocks[2][me] = merged(vtq, vlq, vhq, cut, width)
    pl.semaphore_wait(barrier, 5)

    def copy(axis, side, item, there):
        kind, dx, dz = item
        if kind == "sum_x":
            ref = sums.at[tp, row(dx, 0)]
        elif kind == "sum_z":
            ref = sums.at[tp, pl.ds(((mz - dz + Z) % Z) * X, X)]
        else:
            ref = blocks[kind].at[row(dx, dz)]
        target = row(-side, 0) if axis == "x" else row(0, -side)
        n = places[there]
        return pltpu.make_async_remote_copy(
            src_ref=ref,
            dst_ref=ref,
            send_sem=send_sem.at[n],
            recv_sem=recv_sem.at[n],
            device_id={"rows": target},
            device_id_type=MESH,
        )

    def landed(item):
        kind, dx, dz = item
        if kind == "sum_x":
            ref = sums.at[tp, row(dx, 0)]
        elif kind == "sum_z":
            ref = sums.at[tp, pl.ds(((mz - dz + Z) % Z) * X, X)]
        else:
            ref = blocks[kind].at[row(dx, dz)]
        n = places[item]
        return pltpu.make_async_remote_copy(
            src_ref=ref,
            dst_ref=ref,
            send_sem=send_sem.at[n],
            recv_sem=recv_sem.at[n],
            device_id={"rows": row(1, 0)},
            device_id_type=MESH,
        )

    def turn(kind, pair):
        both = blocks[kind][pl.ds(pair * 2, 2)]
        rows, columns = both.shape[1], both.shape[2]
        lanes = pl.ds(pl.multiple_of(pair * 2 * rows, 2 * rows), 2 * rows)
        flat = both.reshape(2 * rows, columns)
        if kind == 0:
            oq[:columns, lanes] = flat.T
        elif kind == 1:
            ok[:, lanes] = flat[:, :kv].T
            ov[:, lanes] = flat[:, kv:].T
        else:
            oq[cut:, lanes] = flat.T

    sent, swap = [], None
    here = {(kind, dz): {0} if dz == 0 else set() for kind in range(len(PIECES)) for dz in range(Z)}
    for step in steps:
        if step[0] == "send":
            c = copy(*step[1:])
            c.start()
            sent.append(c)
        elif step[0] == "swap":
            swap = pltpu.make_async_remote_copy(
                src_ref=sums.at[tp],
                dst_ref=sums.at[tp],
                send_sem=swap_sem.at[0],
                recv_sem=swap_sem.at[1],
                device_id={"tp": 1 - tp},
                device_id_type=MESH,
            )
            swap.start()
        else:
            item = step[1]
            landed(item).wait_recv()
            kind, dx, dz = item
            if isinstance(kind, str):
                continue
            got = here[kind, dz % Z]
            before = {0, 1, 3} <= got, len(got) == X
            got.add(dx % X)
            after = {0, 1, 3} <= got, len(got) == X
            zz = (mz - dz + Z) % Z
            if after[0] and not before[0]:
                turn(kind, zz * 2 + mx // 2)
            if after[1] and not before[1]:
                turn(kind, zz * 2 + 1 - mx // 2)
    swap.wait()
    g = [sums[i].reshape(Z * X // 2, 2, 128) for i in range(2)]
    parts = [g[j % 2][:, j // 2] for j in range(4)]
    total = parts[0]
    for j in range(1, 4):
        total = total + pltpu.roll(parts[j], 32 * j, axis=1)
    on[...] = total.astype(jnp.bfloat16)
    for c in sent:
        c.wait_send()


def local(tq, lq, hq, tk, lk, hk, tv, lv, hv, nt, ns):
    steps = plan()
    places = {s[4]: i for i, s in enumerate(s for s in steps if s[0] == "send")}
    rows, wide = tq.shape
    kv = tk.shape[1]
    n = Z * X
    args = (tq, lq.T, hq, tk, lk.T, hk, tv, lv.T, hv, nt.reshape(1, -1), ns.reshape(1, -1))
    args = tuple(pltpu.with_memory_space_constraint(a, pltpu.HBM) for a in args)
    q, k, v, norm = pl.pallas_call(
        functools.partial(kernel, steps, places),
        name="gather",
        out_shape=(
            jax.ShapeDtypeStruct((wide, n * rows), jnp.bfloat16),
            jax.ShapeDtypeStruct((kv, n * rows), jnp.bfloat16),
            jax.ShapeDtypeStruct((kv, n * rows), jnp.bfloat16),
            jax.ShapeDtypeStruct((n // 2, 128), jnp.bfloat16),
        ),
        in_specs=[pl.BlockSpec(memory_space=pltpu.HBM)] * 11,
        out_specs=(pl.BlockSpec(memory_space=pltpu.VMEM),) * 4,
        scratch_shapes=[
            *(pltpu.VMEM(a.shape, a.dtype) for a in args),
            *(pltpu.VMEM((n, rows, columns), jnp.bfloat16) for _, columns, _ in PIECES),
            pltpu.VMEM((2, n, 1, 128), jnp.float32),
            pltpu.SemaphoreType.DMA((11,)),
            pltpu.SemaphoreType.DMA((len(places),)),
            pltpu.SemaphoreType.DMA((len(places),)),
            pltpu.SemaphoreType.DMA((2,)),
        ],
        compiler_params=pltpu.CompilerParams(
            collective_id=0, has_side_effects=True, vmem_limit_bytes=24 * 1024 * 1024
        ),
    )(*args)
    return q, k, v, norm.reshape(-1)


def solution(mesh):
    in_specs = (
        P(("job", "rows"), "tp"),
        P(("job", "rows"), None),
        P("job", "tp"),
        P(("job", "rows"), "tp"),
        P(("job", "rows"), None),
        P("job", "tp"),
        P(("job", "rows"), "tp"),
        P(("job", "rows"), None),
        P("job", "tp"),
        P(("job", "rows", "tp")),
        P(("job", "rows", "tp")),
    )
    out_specs = (P(("job", "tp"), None), P(("job", "tp"), None), P(("job", "tp"), None), P("job"))
    return jax.shard_map(local, mesh=mesh, in_specs=in_specs, out_specs=out_specs, check_vma=False)
```

```python
import functools
import heapq
import itertools

import jax
import jax.numpy as jnp
from jax import lax
from jax.experimental import pallas as pl
from jax.experimental.pallas import tpu as pltpu
from jax.sharding import PartitionSpec as P

MESH = pl.DeviceIdType.MESH
mix_rate = 0.5

Z, X = 8, 4
RATE = 46650.0
HOP = 2.0
DEPTH = 2

PIECES = (("x", 640, 1), ("z", 512, 1), ("z", 384, -1))
FIRST = (1, 0, 2)


def onward(d, size, far):
    if d == 0:
        return [(1, 1), (-1, -1)]
    side = 1 if d > 0 else -1
    limit = size // 2 if side == far else size // 2 - 1
    return [(d + side, side)] if abs(d) < limit else []


def forwards(item):
    kind, dx, dz = item
    out = []
    if kind == "sum_x":
        return [("x", s, ("sum_x", n, 0)) for n, s in onward(dx, X, 1)]
    if kind == "sum_z":
        return [("z", s, ("sum_z", 0, n)) for n, s in onward(dz, Z, 1)]
    axis, _, far = PIECES[kind]
    if axis == "x":
        if dz == 0:
            out += [("x", s, (kind, n, 0)) for n, s in onward(dx, X, far)]
        out += [("z", s, (kind, dx, n)) for n, s in onward(dz, Z, 1 if dx % 2 == 0 else -1)]
    else:
        if dx == 0:
            out += [("z", s, (kind, 0, n)) for n, s in onward(dz, Z, far)]
        out += [("x", s, (kind, n, dz)) for n, s in onward(dx, X, 1 if dz % 2 == 0 else -1)]
    return out


def left_to_go(item):
    after = forwards(item)
    return 1 + max(left_to_go(n) for _, _, n in after) if after else 0


def plan():
    links = {(a, s): [] for a in "xz" for s in (1, -1)}
    given = {k: [] for k in links}
    events, tick, steps = [], itertools.count(), []
    norm_x, norm_z = 1, 1

    def cost(item):
        return (512 if isinstance(item[0], str) else PIECES[item[0]][1] * 128) / RATE

    def offer(item):
        for axis, side, there in forwards(item):
            rank = -1000 if isinstance(item[0], str) else -left_to_go(there)
            links[axis, side].append((rank, next(tick), item, there))

    def begin(k, now):
        item = given[k][0]
        heapq.heappush(events, (now + cost(item), next(tick), "done", k, item))

    def feed(now):
        for k in links:
            while links[k] and len(given[k]) < DEPTH:
                links[k].sort()
                _, _, item, there = links[k].pop(0)
                steps.append(("send", k[0], k[1], item, there))
                given[k].append(there)
                if len(given[k]) == 1:
                    begin(k, now)

    offer(("sum_x", 0, 0))
    for kind in FIRST:
        offer((kind, 0, 0))
    feed(0.0)
    while events:
        now, _, what, k, item = heapq.heappop(events)
        if what == "done":
            given[k].pop(0)
            if given[k]:
                begin(k, now)
            heapq.heappush(events, (now + HOP, next(tick), "here", k, item))
            feed(now)
            continue
        steps.append(("wait", item))
        if item[0] == "sum_x":
            norm_x += 1
            if norm_x == X:
                offer(("sum_z", 0, 0))
        elif item[0] == "sum_z":
            norm_z += 1
        offer(item)
        feed(now)
        if item[0] == "sum_z" and norm_z == Z:
            steps.append(("swap",))
    return steps


def kernel(
    steps, places, tq, lq, hq, tk, lk, hk, tv, lv, hv, nt, ns, oq, ok, ov, on, *scratch
):
    vin, blocks, sums = scratch[:11], scratch[11 : 11 + len(PIECES)], scratch[11 + len(PIECES)]
    in_sem, send_sem, recv_sem, swap_sem = scratch[12 + len(PIECES) :]
    me, tp = lax.axis_index("rows"), lax.axis_index("tp")
    mz, mx = me // X, me % X

    def row(dx, dz):
        return ((mz - dz + Z) % Z) * X + (mx - dx + X) % X

    loads = [
        pltpu.make_async_copy(a, b, in_sem.at[i])
        for i, (a, b) in enumerate(zip((tq, lq, hq, tk, lk, hk, tv, lv, hv, nt, ns), vin))
    ]
    for load in loads:
        load.start()

    barrier = pltpu.get_barrier_semaphore()
    for there in (row(1, 0), row(-1, 0), row(0, 1), row(0, -1)):
        pl.semaphore_signal(barrier, inc=1, device_id={"rows": there}, device_id_type=MESH)
    pl.semaphore_signal(barrier, inc=1, device_id={"tp": 1 - tp}, device_id_type=MESH)

    for load in loads:
        load.wait()
    vtq, vlq, vhq, vtk, vlk, vhk, vtv, vlv, vhv, vnt, vns = vin

    def merged(train, low, high, lo, hi):
        product = lax.dot_general(
            low[...], high[:, lo:hi], (((0,), (0,)), ((), ())), preferred_element_type=jnp.float32
        )
        return (train[:, lo:hi].astype(jnp.float32) + mix_rate * product).astype(jnp.bfloat16)

    cut = PIECES[0][1]
    width = vtq.shape[1]
    kv = vtk.shape[1]
    sums[tp, me] = jnp.concatenate(
        [vnt[...] + vns[...], jnp.zeros((1, 128 - vnt.shape[1]), jnp.float32)], axis=1
    )
    blocks[1][me, :, :kv] = merged(vtk, vlk, vhk, 0, kv)
    blocks[1][me, :, kv:] = merged(vtv, vlv, vhv, 0, kv)
    blocks[0][me] = merged(vtq, vlq, vhq, 0, cut)
    blocks[2][me] = merged(vtq, vlq, vhq, cut, width)
    pl.semaphore_wait(barrier, 5)

    def copy(axis, side, item, there):
        kind, dx, dz = item
        if kind == "sum_x":
            ref = sums.at[tp, row(dx, 0)]
        elif kind == "sum_z":
            ref = sums.at[tp, pl.ds(((mz - dz + Z) % Z) * X, X)]
        else:
            ref = blocks[kind].at[row(dx, dz)]
        target = row(-side, 0) if axis == "x" else row(0, -side)
        n = places[there]
        return pltpu.make_async_remote_copy(
            src_ref=ref,
            dst_ref=ref,
            send_sem=send_sem.at[n],
            recv_sem=recv_sem.at[n],
            device_id={"rows": target},
            device_id_type=MESH,
        )

    def landed(item):
        kind, dx, dz = item
        if kind == "sum_x":
            ref = sums.at[tp, row(dx, 0)]
        elif kind == "sum_z":
            ref = sums.at[tp, pl.ds(((mz - dz + Z) % Z) * X, X)]
        else:
            ref = blocks[kind].at[row(dx, dz)]
        n = places[item]
        return pltpu.make_async_remote_copy(
            src_ref=ref,
            dst_ref=ref,
            send_sem=send_sem.at[n],
            recv_sem=recv_sem.at[n],
            device_id={"rows": row(1, 0)},
            device_id_type=MESH,
        )

    def turn(kind, pair):
        both = blocks[kind][pl.ds(pair * 2, 2)]
        rows, columns = both.shape[1], both.shape[2]
        lanes = pl.ds(pl.multiple_of(pair * 2 * rows, 2 * rows), 2 * rows)
        flat = both.reshape(2 * rows, columns)
        if kind == 0:
            oq[:columns, lanes] = flat.T
        elif kind == 1:
            ok[:, lanes] = flat[:, :kv].T
            ov[:, lanes] = flat[:, kv:].T
        else:
            oq[cut:, lanes] = flat.T

    sent, swap = [], None
    here = {(kind, dz): {0} if dz == 0 else set() for kind in range(len(PIECES)) for dz in range(Z)}
    for step in steps:
        if step[0] == "send":
            c = copy(*step[1:])
            c.start()
            sent.append(c)
        elif step[0] == "swap":
            swap = pltpu.make_async_remote_copy(
                src_ref=sums.at[tp],
                dst_ref=sums.at[tp],
                send_sem=swap_sem.at[0],
                recv_sem=swap_sem.at[1],
                device_id={"tp": 1 - tp},
                device_id_type=MESH,
            )
            swap.start()
        else:
            item = step[1]
            landed(item).wait_recv()
            kind, dx, dz = item
            if isinstance(kind, str):
                continue
            got = here[kind, dz % Z]
            before = {0, 1, 3} <= got, len(got) == X
            got.add(dx % X)
            after = {0, 1, 3} <= got, len(got) == X
            zz = (mz - dz + Z) % Z
            if after[0] and not before[0]:
                turn(kind, zz * 2 + mx // 2)
            if after[1] and not before[1]:
                turn(kind, zz * 2 + 1 - mx // 2)
    swap.wait()
    g = [sums[i].reshape(Z * X // 2, 2, 128) for i in range(2)]
    parts = [g[j % 2][:, j // 2] for j in range(4)]
    total = parts[0]
    for j in range(1, 4):
        total = total + pltpu.roll(parts[j], 32 * j, axis=1)
    on[...] = total.astype(jnp.bfloat16)
    for c in sent:
        c.wait_send()


def write_out(*refs):
    n = len(refs) // 2
    sem = refs[-1]
    copies = [pltpu.make_async_copy(refs[i], refs[n + i], sem.at[i]) for i in range(n)]
    for c in copies:
        c.start()
    for c in copies:
        c.wait()


def local(tq, lq, hq, tk, lk, hk, tv, lv, hv, nt, ns):
    steps = plan()
    places = {s[4]: i for i, s in enumerate(s for s in steps if s[0] == "send")}
    rows, wide = tq.shape
    kv = tk.shape[1]
    n = Z * X
    args = (tq, lq.T, hq, tk, lk.T, hk, tv, lv.T, hv, nt.reshape(1, -1), ns.reshape(1, -1))
    args = tuple(pltpu.with_memory_space_constraint(a, pltpu.HBM) for a in args)
    q, k, v, norm = pl.pallas_call(
        functools.partial(kernel, steps, places),
        name="gather",
        out_shape=(
            jax.ShapeDtypeStruct((wide, n * rows), jnp.bfloat16),
            jax.ShapeDtypeStruct((kv, n * rows), jnp.bfloat16),
            jax.ShapeDtypeStruct((kv, n * rows), jnp.bfloat16),
            jax.ShapeDtypeStruct((n // 2, 128), jnp.bfloat16),
        ),
        in_specs=[pl.BlockSpec(memory_space=pltpu.HBM)] * 11,
        out_specs=(pl.BlockSpec(memory_space=pltpu.VMEM),) * 4,
        scratch_shapes=[
            *(pltpu.VMEM(a.shape, a.dtype) for a in args),
            *(pltpu.VMEM((n, rows, columns), jnp.bfloat16) for _, columns, _ in PIECES),
            pltpu.VMEM((2, n, 1, 128), jnp.float32),
            pltpu.SemaphoreType.DMA((11,)),
            pltpu.SemaphoreType.DMA((len(places),)),
            pltpu.SemaphoreType.DMA((len(places),)),
            pltpu.SemaphoreType.DMA((2,)),
        ],
        compiler_params=pltpu.CompilerParams(
            collective_id=0, has_side_effects=True, vmem_limit_bytes=24 * 1024 * 1024
        ),
    )(*args)
    held = tuple(pltpu.with_memory_space_constraint(a, pltpu.VMEM) for a in (q, k, v, norm))
    q, k, v, norm = pl.pallas_call(
        write_out,
        name="write",
        out_shape=tuple(jax.ShapeDtypeStruct(a.shape, a.dtype) for a in held),
        in_specs=[pl.BlockSpec(memory_space=pltpu.VMEM)] * 4,
        out_specs=(pl.BlockSpec(memory_space=pltpu.HBM),) * 4,
        scratch_shapes=[pltpu.SemaphoreType.DMA((4,))],
        compiler_params=pltpu.CompilerParams(vmem_limit_bytes=1024 * 1024),
    )(*held)
    return q, k, v, norm.reshape(-1)


def solution(mesh):
    in_specs = (
        P(("job", "rows"), "tp"),
        P(("job", "rows"), None),
        P("job", "tp"),
        P(("job", "rows"), "tp"),
        P(("job", "rows"), None),
        P("job", "tp"),
        P(("job", "rows"), "tp"),
        P(("job", "rows"), None),
        P("job", "tp"),
        P(("job", "rows", "tp")),
        P(("job", "rows", "tp")),
    )
    out_specs = (P(("job", "tp"), None), P(("job", "tp"), None), P(("job", "tp"), None), P("job"))
    return jax.shard_map(local, mesh=mesh, in_specs=in_specs, out_specs=out_specs, check_vma=False)
```

```python
import functools
import heapq
import itertools

import jax
import jax.numpy as jnp
from jax import lax
from jax.experimental import pallas as pl
from jax.experimental.pallas import tpu as pltpu
from jax.sharding import PartitionSpec as P

MESH = pl.DeviceIdType.MESH
mix_rate = 0.5

Z, X = 8, 4
RATE = 46650.0
HOP = 2.0
DEPTH = 2

PIECES = (("x", 640, 1), ("z", 512, 1), ("z", 384, -1))
FIRST = (1, 0, 2)


def onward(d, size, far):
    if d == 0:
        return [(1, 1), (-1, -1)]
    side = 1 if d > 0 else -1
    limit = size // 2 if side == far else size // 2 - 1
    return [(d + side, side)] if abs(d) < limit else []


def forwards(item):
    kind, dx, dz = item
    out = []
    if kind == "sum_x":
        return [("x", s, ("sum_x", n, 0)) for n, s in onward(dx, X, 1)]
    if kind == "sum_z":
        return [("z", s, ("sum_z", 0, n)) for n, s in onward(dz, Z, 1)]
    axis, _, far = PIECES[kind]
    if axis == "x":
        if dz == 0:
            out += [("x", s, (kind, n, 0)) for n, s in onward(dx, X, far)]
        out += [("z", s, (kind, dx, n)) for n, s in onward(dz, Z, 1 if dx % 2 == 0 else -1)]
    else:
        if dx == 0:
            out += [("z", s, (kind, 0, n)) for n, s in onward(dz, Z, far)]
        out += [("x", s, (kind, n, dz)) for n, s in onward(dx, X, 1 if dz % 2 == 0 else -1)]
    return out


def left_to_go(item):
    after = forwards(item)
    return 1 + max(left_to_go(n) for _, _, n in after) if after else 0


def plan():
    links = {(a, s): [] for a in "xz" for s in (1, -1)}
    given = {k: [] for k in links}
    events, tick, steps = [], itertools.count(), []
    norm_x, norm_z = 1, 1

    def cost(item):
        return (512 if isinstance(item[0], str) else PIECES[item[0]][1] * 128) / RATE

    def offer(item):
        for axis, side, there in forwards(item):
            rank = -1000 if isinstance(item[0], str) else -left_to_go(there)
            links[axis, side].append((rank, next(tick), item, there))

    def begin(k, now):
        item = given[k][0]
        heapq.heappush(events, (now + cost(item), next(tick), "done", k, item))

    def feed(now):
        for k in links:
            while links[k] and len(given[k]) < DEPTH:
                links[k].sort()
                _, _, item, there = links[k].pop(0)
                steps.append(("send", k[0], k[1], item, there))
                given[k].append(there)
                if len(given[k]) == 1:
                    begin(k, now)

    offer(("sum_x", 0, 0))
    for kind in FIRST:
        offer((kind, 0, 0))
    feed(0.0)
    while events:
        now, _, what, k, item = heapq.heappop(events)
        if what == "done":
            given[k].pop(0)
            if given[k]:
                begin(k, now)
            heapq.heappush(events, (now + HOP, next(tick), "here", k, item))
            feed(now)
            continue
        steps.append(("wait", item))
        if item[0] == "sum_x":
            norm_x += 1
            if norm_x == X:
                offer(("sum_z", 0, 0))
        elif item[0] == "sum_z":
            norm_z += 1
        offer(item)
        feed(now)
        if item[0] == "sum_z" and norm_z == Z:
            steps.append(("swap",))
    return steps


def kernel(
    steps, places, tq, lq, hq, tk, lk, hk, tv, lv, hv, nt, ns, oq, ok, ov, on, *scratch
):
    vin, blocks, sums = scratch[:11], scratch[11 : 11 + len(PIECES)], scratch[11 + len(PIECES)]
    in_sem, send_sem, recv_sem, swap_sem = scratch[12 + len(PIECES) :]
    me, tp = lax.axis_index("rows"), lax.axis_index("tp")
    mz, mx = me // X, me % X

    def row(dx, dz):
        return ((mz - dz + Z) % Z) * X + (mx - dx + X) % X

    barrier = pltpu.get_barrier_semaphore()
    for there in (row(1, 0), row(-1, 0), row(0, 1), row(0, -1)):
        pl.semaphore_signal(barrier, inc=1, device_id={"rows": there}, device_id_type=MESH)
    pl.semaphore_signal(barrier, inc=1, device_id={"tp": 1 - tp}, device_id_type=MESH)

    loads = [
        pltpu.make_async_copy(a, b, in_sem.at[i])
        for i, (a, b) in enumerate(zip((tq, lq, hq, tk, lk, hk, tv, lv, hv, nt, ns), vin))
    ]
    for load in loads[3:] + loads[:3]:
        load.start()
    for load in loads[3:]:
        load.wait()
    vtq, vlq, vhq, vtk, vlk, vhk, vtv, vlv, vhv, vnt, vns = vin

    def merged(train, low, high, lo, hi):
        product = lax.dot_general(
            low[...], high[:, lo:hi], (((0,), (0,)), ((), ())), preferred_element_type=jnp.float32
        )
        return (train[:, lo:hi].astype(jnp.float32) + mix_rate * product).astype(jnp.bfloat16)

    cut = PIECES[0][1]
    width = vtq.shape[1]
    kv = vtk.shape[1]
    sums[tp, me] = jnp.concatenate(
        [vnt[...] + vns[...], jnp.zeros((1, 128 - vnt.shape[1]), jnp.float32)], axis=1
    )
    blocks[1][me, :, :kv] = merged(vtk, vlk, vhk, 0, kv)
    blocks[1][me, :, kv:] = merged(vtv, vlv, vhv, 0, kv)
    pl.semaphore_wait(barrier, 5)

    def merge_query():
        for load in loads[:3]:
            load.wait()
        blocks[0][me] = merged(vtq, vlq, vhq, 0, cut)
        blocks[2][me] = merged(vtq, vlq, vhq, cut, width)

    def send_sem_of(kind):
        return send_sem.at[("sum_x", "sum_z").index(kind) + len(PIECES) if isinstance(kind, str) else kind]

    def all_sent(kind):
        count = Z * X - 1
        if kind == "sum_x":
            ref = sums.at[tp, pl.ds(0, X - 1)]
        elif kind == "sum_z":
            ref = sums.at[tp, pl.ds(0, (Z - 1) * X)]
        else:
            ref = blocks[kind].at[pl.ds(0, count)]
        pltpu.make_async_remote_copy(
            src_ref=ref,
            dst_ref=ref,
            send_sem=send_sem_of(kind),
            recv_sem=recv_sem.at[0],
            device_id={"rows": row(1, 0)},
            device_id_type=MESH,
        ).wait_send()

    def copy(axis, side, item, there):
        kind, dx, dz = item
        if kind == "sum_x":
            ref = sums.at[tp, row(dx, 0)]
        elif kind == "sum_z":
            ref = sums.at[tp, pl.ds(((mz - dz + Z) % Z) * X, X)]
        else:
            ref = blocks[kind].at[row(dx, dz)]
        target = row(-side, 0) if axis == "x" else row(0, -side)
        n = places[there]
        return pltpu.make_async_remote_copy(
            src_ref=ref,
            dst_ref=ref,
            send_sem=send_sem_of(kind),
            recv_sem=recv_sem.at[n],
            device_id={"rows": target},
            device_id_type=MESH,
        )

    def landed(item):
        kind, dx, dz = item
        if kind == "sum_x":
            ref = sums.at[tp, row(dx, 0)]
        elif kind == "sum_z":
            ref = sums.at[tp, pl.ds(((mz - dz + Z) % Z) * X, X)]
        else:
            ref = blocks[kind].at[row(dx, dz)]
        n = places[item]
        return pltpu.make_async_remote_copy(
            src_ref=ref,
            dst_ref=ref,
            send_sem=send_sem_of(kind),
            recv_sem=recv_sem.at[n],
            device_id={"rows": row(1, 0)},
            device_id_type=MESH,
        )

    def turn(kind, pair):
        both = blocks[kind][pl.ds(pair * 2, 2)]
        rows, columns = both.shape[1], both.shape[2]
        lanes = pl.ds(pl.multiple_of(pair * 2 * rows, 2 * rows), 2 * rows)
        flat = both.reshape(2 * rows, columns)
        if kind == 0:
            oq[:columns, lanes] = flat.T
        elif kind == 1:
            ok[:, lanes] = flat[:, :kv].T
            ov[:, lanes] = flat[:, kv:].T
        else:
            oq[cut:, lanes] = flat.T

    def join_norm():
        g = [sums[i].reshape(Z * X // 2, 2, 128) for i in range(2)]
        parts = [g[j % 2][:, j // 2] for j in range(4)]
        total = parts[0]
        for j in range(1, 4):
            total = total + pltpu.roll(parts[j], 32 * j, axis=1)
        on[...] = total.astype(jnp.bfloat16)

    swap, late = None, len(steps) - 16
    ready = {1}
    here = {(kind, dz): {0} if dz == 0 else set() for kind in range(len(PIECES)) for dz in range(Z)}
    for at, step in enumerate(steps):
        if at == late:
            swap.wait()
            join_norm()
        if step[0] == "send":
            kind, dx, dz = step[3]
            if kind in (0, 2) and kind not in ready and (dx, dz) == (0, 0):
                merge_query()
                ready = {0, 1, 2}
            copy(*step[1:]).start()
        elif step[0] == "swap":
            swap = pltpu.make_async_remote_copy(
                src_ref=sums.at[tp],
                dst_ref=sums.at[tp],
                send_sem=swap_sem.at[0],
                recv_sem=swap_sem.at[1],
                device_id={"tp": 1 - tp},
                device_id_type=MESH,
            )
            swap.start()
        else:
            item = step[1]
            landed(item).wait_recv()
            kind, dx, dz = item
            if isinstance(kind, str):
                continue
            got = here[kind, dz % Z]
            before = {0, 1, 3} <= got, len(got) == X
            got.add(dx % X)
            after = {0, 1, 3} <= got, len(got) == X
            zz = (mz - dz + Z) % Z
            if after[0] and not before[0]:
                turn(kind, zz * 2 + mx // 2)
            if after[1] and not before[1]:
                turn(kind, zz * 2 + 1 - mx // 2)
    for kind in ("sum_x", "sum_z", *range(len(PIECES))):
        all_sent(kind)


def write_out(*refs):
    n = len(refs) // 2
    sem = refs[-1]
    copies = [pltpu.make_async_copy(refs[i], refs[n + i], sem.at[i]) for i in range(n)]
    for c in copies:
        c.start()
    for c in copies:
        c.wait()


def local(tq, lq, hq, tk, lk, hk, tv, lv, hv, nt, ns):
    steps = plan()
    places = {s[4]: i for i, s in enumerate(s for s in steps if s[0] == "send")}
    rows, wide = tq.shape
    kv = tk.shape[1]
    n = Z * X
    args = (tq, lq.T, hq, tk, lk.T, hk, tv, lv.T, hv, nt.reshape(1, -1), ns.reshape(1, -1))
    args = tuple(pltpu.with_memory_space_constraint(a, pltpu.HBM) for a in args)
    q, k, v, norm = pl.pallas_call(
        functools.partial(kernel, steps, places),
        name="gather",
        out_shape=(
            jax.ShapeDtypeStruct((wide, n * rows), jnp.bfloat16),
            jax.ShapeDtypeStruct((kv, n * rows), jnp.bfloat16),
            jax.ShapeDtypeStruct((kv, n * rows), jnp.bfloat16),
            jax.ShapeDtypeStruct((n // 2, 128), jnp.bfloat16),
        ),
        in_specs=[pl.BlockSpec(memory_space=pltpu.HBM)] * 11,
        out_specs=(pl.BlockSpec(memory_space=pltpu.VMEM),) * 4,
        scratch_shapes=[
            *(pltpu.VMEM(a.shape, a.dtype) for a in args),
            *(pltpu.VMEM((n, rows, columns), jnp.bfloat16) for _, columns, _ in PIECES),
            pltpu.VMEM((2, n, 1, 128), jnp.float32),
            pltpu.SemaphoreType.DMA((11,)),
            pltpu.SemaphoreType.DMA((len(PIECES) + 2,)),
            pltpu.SemaphoreType.DMA((len(places),)),
            pltpu.SemaphoreType.DMA((2,)),
        ],
        compiler_params=pltpu.CompilerParams(
            collective_id=0, has_side_effects=True, vmem_limit_bytes=24 * 1024 * 1024
        ),
    )(*args)
    held = tuple(pltpu.with_memory_space_constraint(a, pltpu.VMEM) for a in (q, k, v, norm))
    q, k, v, norm = pl.pallas_call(
        write_out,
        name="write",
        out_shape=tuple(jax.ShapeDtypeStruct(a.shape, a.dtype) for a in held),
        in_specs=[pl.BlockSpec(memory_space=pltpu.VMEM)] * 4,
        out_specs=(pl.BlockSpec(memory_space=pltpu.HBM),) * 4,
        scratch_shapes=[pltpu.SemaphoreType.DMA((4,))],
        compiler_params=pltpu.CompilerParams(vmem_limit_bytes=1024 * 1024),
    )(*held)
    return q, k, v, norm.reshape(-1)


def solution(mesh):
    in_specs = (
        P(("job", "rows"), "tp"),
        P(("job", "rows"), None),
        P("job", "tp"),
        P(("job", "rows"), "tp"),
        P(("job", "rows"), None),
        P("job", "tp"),
        P(("job", "rows"), "tp"),
        P(("job", "rows"), None),
        P("job", "tp"),
        P(("job", "rows", "tp")),
        P(("job", "rows", "tp")),
    )
    out_specs = (P(("job", "tp"), None), P(("job", "tp"), None), P(("job", "tp"), None), P("job"))
    return jax.shard_map(local, mesh=mesh, in_specs=in_specs, out_specs=out_specs, check_vma=False)
```

```python
import functools
import heapq
import itertools

import jax
import jax.numpy as jnp
from jax import lax
from jax.experimental import pallas as pl
from jax.experimental.pallas import tpu as pltpu
from jax.sharding import PartitionSpec as P

MESH = pl.DeviceIdType.MESH
mix_rate = 0.5

Z, X = 8, 4
RATE = 46650.0
HOP = 2.0
DEPTH = 3

MEET = 8

PIECES = (("z", 512, -1), ("x", 384, 1), ("x", 256, -1), ("z", 384, 1))
SPANS = (((1, 0, 256), (2, 0, 256)), ((0, 0, 384),), ((0, 384, 640),), ((0, 640, 1024),))
FIRST = (0, 1, 2, 3)
UP = ((0, 1), (2, 1), (1, 2))


def onward(d, size, far):
    if d == 0:
        return [(1, 1), (-1, -1)]
    side = 1 if d > 0 else -1
    limit = size // 2 if side == far else size // 2 - 1
    return [(d + side, side)] if abs(d) < limit else []


def forwards(item):
    kind, dx, dz = item
    out = []
    if kind == "sum_x":
        return [("x", s, ("sum_x", n, 0)) for n, s in onward(dx, X, 1)]
    if kind == "sum_z":
        return [("z", s, ("sum_z", 0, n)) for n, s in onward(dz, Z, 1)]
    axis, _, far = PIECES[kind]
    if axis == "x":
        if dz == 0:
            out += [("x", s, (kind, n, 0)) for n, s in onward(dx, X, far)]
        out += [("z", s, (kind, dx, n)) for n, s in onward(dz, Z, 1 if (dx % X, kind) in UP else -1)]
    else:
        if dx == 0:
            out += [("z", s, (kind, 0, n)) for n, s in onward(dz, Z, far)]
        out += [("x", s, (kind, n, dz)) for n, s in onward(dx, X, 1 if dz % 2 == 0 else -1)]
    return out


def left_to_go(item):
    after = forwards(item)
    return 1 + max(left_to_go(n) for _, _, n in after) if after else 0


def plan():
    links = {(a, s): [] for a in "xz" for s in (1, -1)}
    given = {k: [] for k in links}
    events, tick, steps = [], itertools.count(), []
    norm_x, norm_z, waits = 1, 1, 0

    def cost(item):
        return (1024 if isinstance(item[0], str) else PIECES[item[0]][1] * 128) / RATE

    def offer(item):
        for axis, side, there in forwards(item):
            rank = -1000 if isinstance(item[0], str) else -left_to_go(there)
            links[axis, side].append((rank, next(tick), item, there))

    def begin(k, now):
        item = given[k][0]
        heapq.heappush(events, (now + cost(item), next(tick), "done", k, item))

    def feed(now):
        for k in links:
            while links[k] and len(given[k]) < DEPTH:
                links[k].sort()
                _, _, item, there = links[k].pop(0)
                steps.append(("send", k[0], k[1], item, there))
                given[k].append(there)
                if len(given[k]) == 1:
                    begin(k, now)

    for kind in FIRST:
        offer((kind, 0, 0))
    feed(0.0)
    while events:
        now, _, what, k, item = heapq.heappop(events)
        if what == "done":
            given[k].pop(0)
            if given[k]:
                begin(k, now)
            heapq.heappush(events, (now + HOP, next(tick), "here", k, item))
            feed(now)
            continue
        steps.append(("wait", item))
        waits += 1
        if waits == MEET:
            steps.append(("meet",))
            offer(("sum_x", 0, 0))
        if item[0] == "sum_x":
            norm_x += 1
            if norm_x == X:
                offer(("sum_z", 0, 0))
        elif item[0] == "sum_z":
            norm_z += 1
        offer(item)
        feed(now)
        if item[0] == "sum_z" and norm_z == Z:
            steps.append(("join",))
    return steps


def kernel(
    steps, places, tq, lq, hq, tk, lk, hk, tv, lv, hv, nt, ns, oq, ok, ov, on, *scratch
):
    vin, blocks, sums = scratch[:11], scratch[11 : 11 + len(PIECES)], scratch[11 + len(PIECES)]
    in_sem, send_sem, recv_sem, pair_sem = scratch[12 + len(PIECES) :]
    me, tp = lax.axis_index("rows"), lax.axis_index("tp")
    mz, mx = me // X, me % X

    def row(dx, dz):
        return ((mz - dz + Z) % Z) * X + (mx - dx + X) % X

    barrier = pltpu.get_barrier_semaphore()
    for there in (row(1, 0), row(-1, 0), row(0, 1), row(0, -1)):
        pl.semaphore_signal(barrier, inc=1, device_id={"rows": there}, device_id_type=MESH)

    @pl.when(tp == 0)
    def _():
        pl.semaphore_signal(barrier, inc=1, device_id={"tp": 1}, device_id_type=MESH)


    loads = [
        pltpu.make_async_copy(a, b, in_sem.at[i])
        for i, (a, b) in enumerate(zip((tq, lq, hq, tk, lk, hk, tv, lv, hv, nt, ns), vin))
    ]
    for load in loads[3:] + loads[:3]:
        load.start()
    for load in loads[3:]:
        load.wait()
    vtq, vlq, vhq, vtk, vlk, vhk, vtv, vlv, vhv, vnt, vns = vin

    def merged(train, low, high, lo, hi):
        product = lax.dot_general(
            low[...], high[:, lo:hi], (((0,), (0,)), ((), ())), preferred_element_type=jnp.float32
        )
        return (train[:, lo:hi].astype(jnp.float32) + mix_rate * product).astype(jnp.bfloat16)

    sources = ((vtq, vlq, vhq), (vtk, vlk, vhk), (vtv, vlv, vhv))
    outs = (oq, ok, ov)

    def merge(kind):
        at = 0
        for array, lo, hi in SPANS[kind]:
            blocks[kind][me, :, at : at + hi - lo] = merged(*sources[array], lo, hi)
            at += hi - lo

    def merge_query():
        for load in loads[:3]:
            load.wait()
        for kind in range(1, len(PIECES)):
            merge(kind)

    sums[me, tp] = jnp.concatenate(
        [vnt[...] + vns[...], jnp.zeros((1, 128 - vnt.shape[1]), jnp.float32)], axis=1
    )
    merge(0)
    pl.semaphore_wait(barrier, 4 + tp)

    def pair_copy(core):
        return pltpu.make_async_remote_copy(
            src_ref=sums.at[me, core],
            dst_ref=sums.at[me, core],
            send_sem=pair_sem.at[0],
            recv_sem=pair_sem.at[1],
            device_id={"tp": 1 - tp},
            device_id_type=MESH,
        )

    @pl.when(tp == 1)
    def _():
        pair_copy(1).start()

    def send_sem_of(kind):
        return send_sem.at[("sum_x", "sum_z").index(kind) + len(PIECES) if isinstance(kind, str) else kind]

    def all_sent(kind):
        count = Z * X - 1
        if kind == "sum_x":
            ref = sums.at[pl.ds(0, X - 1)]
        elif kind == "sum_z":
            ref = sums.at[pl.ds(0, (Z - 1) * X)]
        else:
            ref = blocks[kind].at[pl.ds(0, count)]
        pltpu.make_async_remote_copy(
            src_ref=ref,
            dst_ref=ref,
            send_sem=send_sem_of(kind),
            recv_sem=recv_sem.at[0],
            device_id={"rows": row(1, 0)},
            device_id_type=MESH,
        ).wait_send()

    def copy(axis, side, item, there):
        kind, dx, dz = item
        if kind == "sum_x":
            ref = sums.at[row(dx, 0)]
        elif kind == "sum_z":
            ref = sums.at[pl.ds(((mz - dz + Z) % Z) * X, X)]
        else:
            ref = blocks[kind].at[row(dx, dz)]
        target = row(-side, 0) if axis == "x" else row(0, -side)
        n = places[there]
        return pltpu.make_async_remote_copy(
            src_ref=ref,
            dst_ref=ref,
            send_sem=send_sem_of(kind),
            recv_sem=recv_sem.at[n],
            device_id={"rows": target},
            device_id_type=MESH,
        )

    def landed(item):
        kind, dx, dz = item
        if kind == "sum_x":
            ref = sums.at[row(dx, 0)]
        elif kind == "sum_z":
            ref = sums.at[pl.ds(((mz - dz + Z) % Z) * X, X)]
        else:
            ref = blocks[kind].at[row(dx, dz)]
        n = places[item]
        return pltpu.make_async_remote_copy(
            src_ref=ref,
            dst_ref=ref,
            send_sem=send_sem_of(kind),
            recv_sem=recv_sem.at[n],
            device_id={"rows": row(1, 0)},
            device_id_type=MESH,
        )

    def turn(kind, pair):
        both = blocks[kind][pl.ds(pair * 2, 2)]
        rows, columns = both.shape[1], both.shape[2]
        lanes = pl.ds(pl.multiple_of(pair * 2 * rows, 2 * rows), 2 * rows)
        flat = both.reshape(2 * rows, columns)
        at = 0
        for array, lo, hi in SPANS[kind]:
            outs[array][lo:hi, lanes] = flat[:, at : at + hi - lo].T
            at += hi - lo

    def join_norm():
        parts = sums[...].reshape(Z * X // 2, 4, 128)
        total = parts[:, 0]
        for j in range(1, 4):
            total = total + pltpu.roll(parts[:, j], 32 * j, axis=1)
        on[...] = total.astype(jnp.bfloat16)

    merged_all = False
    here = {(kind, dz): {0} if dz == 0 else set() for kind in range(len(PIECES)) for dz in range(Z)}
    for step in steps:
        if step[0] == "send":
            kind, dx, dz = step[3]
            if not (merged_all or isinstance(kind, str) or kind == 0):
                merge_query()
                merged_all = True
            copy(*step[1:]).start()
        elif step[0] == "meet":

            @pl.when(tp == 0)
            def _():
                pair_copy(1).wait_recv()
                pair_copy(0).start()

            @pl.when(tp == 1)
            def _():
                pair_copy(0).wait_recv()

        elif step[0] == "join":
            join_norm()
        else:
            item = step[1]
            landed(item).wait_recv()
            kind, dx, dz = item
            if isinstance(kind, str):
                continue
            got = here[kind, dz % Z]
            before = {0, 1, 3} <= got, len(got) == X
            got.add(dx % X)
            after = {0, 1, 3} <= got, len(got) == X
            zz = (mz - dz + Z) % Z
            if after[0] and not before[0]:
                turn(kind, zz * 2 + mx // 2)
            if after[1] and not before[1]:
                turn(kind, zz * 2 + 1 - mx // 2)
    for kind in ("sum_x", "sum_z", *range(len(PIECES))):
        all_sent(kind)
    pair_copy(tp).wait_send()


def write_out(*refs):
    n = len(refs) // 2
    sem = refs[-1]
    copies = [pltpu.make_async_copy(refs[i], refs[n + i], sem.at[i]) for i in range(n)]
    for c in copies:
        c.start()
    for c in copies:
        c.wait()


def local(tq, lq, hq, tk, lk, hk, tv, lv, hv, nt, ns):
    steps = plan()
    places = {s[4]: i for i, s in enumerate(s for s in steps if s[0] == "send")}
    rows, wide = tq.shape
    kv = tk.shape[1]
    n = Z * X
    args = (tq, lq.T, hq, tk, lk.T, hk, tv, lv.T, hv, nt.reshape(1, -1), ns.reshape(1, -1))
    args = tuple(pltpu.with_memory_space_constraint(a, pltpu.HBM) for a in args)
    q, k, v, norm = pl.pallas_call(
        functools.partial(kernel, steps, places),
        name="gather",
        out_shape=(
            jax.ShapeDtypeStruct((wide, n * rows), jnp.bfloat16),
            jax.ShapeDtypeStruct((kv, n * rows), jnp.bfloat16),
            jax.ShapeDtypeStruct((kv, n * rows), jnp.bfloat16),
            jax.ShapeDtypeStruct((n // 2, 128), jnp.bfloat16),
        ),
        in_specs=[pl.BlockSpec(memory_space=pltpu.HBM)] * 11,
        out_specs=(pl.BlockSpec(memory_space=pltpu.VMEM),) * 4,
        scratch_shapes=[
            *(pltpu.VMEM(a.shape, a.dtype) for a in args),
            *(pltpu.VMEM((n, rows, columns), jnp.bfloat16) for _, columns, _ in PIECES),
            pltpu.VMEM((n, 2, 1, 128), jnp.float32),
            pltpu.SemaphoreType.DMA((11,)),
            pltpu.SemaphoreType.DMA((len(PIECES) + 2,)),
            pltpu.SemaphoreType.DMA((len(places),)),
            pltpu.SemaphoreType.DMA((2,)),
        ],
        compiler_params=pltpu.CompilerParams(
            collective_id=0, has_side_effects=True, vmem_limit_bytes=24 * 1024 * 1024
        ),
    )(*args)
    held = tuple(pltpu.with_memory_space_constraint(a, pltpu.VMEM) for a in (q, k, v, norm))
    q, k, v, norm = pl.pallas_call(
        write_out,
        name="write",
        out_shape=tuple(jax.ShapeDtypeStruct(a.shape, a.dtype) for a in held),
        in_specs=[pl.BlockSpec(memory_space=pltpu.VMEM)] * 4,
        out_specs=(pl.BlockSpec(memory_space=pltpu.HBM),) * 4,
        scratch_shapes=[pltpu.SemaphoreType.DMA((4,))],
        compiler_params=pltpu.CompilerParams(vmem_limit_bytes=1024 * 1024),
    )(*held)
    return q, k, v, norm.reshape(-1)


def solution(mesh):
    in_specs = (
        P(("job", "rows"), "tp"),
        P(("job", "rows"), None),
        P("job", "tp"),
        P(("job", "rows"), "tp"),
        P(("job", "rows"), None),
        P("job", "tp"),
        P(("job", "rows"), "tp"),
        P(("job", "rows"), None),
        P("job", "tp"),
        P(("job", "rows", "tp")),
        P(("job", "rows", "tp")),
    )
    out_specs = (P(("job", "tp"), None), P(("job", "tp"), None), P(("job", "tp"), None), P("job"))
    return jax.shard_map(local, mesh=mesh, in_specs=in_specs, out_specs=out_specs, check_vma=False)
```

```python
import functools
import heapq
import itertools

import jax
import jax.numpy as jnp
from jax import lax
from jax.experimental import pallas as pl
from jax.experimental.pallas import tpu as pltpu
from jax.sharding import PartitionSpec as P

MESH = pl.DeviceIdType.MESH
mix_rate = 0.5

Z, X = 8, 4
RATE = 46650.0
HOP = 2.0
DEPTH = 3

MEET = 8

PIECES = (("z", 512, -1), ("x", 384, 1), ("x", 256, -1), ("z", 384, 1))
SPANS = (((1, 0, 256), (2, 0, 256)), ((0, 0, 384),), ((0, 384, 640),), ((0, 640, 1024),))
FIRST = (0, 1, 2, 3)
UP = ((0, 1), (2, 1), (1, 2))


def onward(d, size, far):
    if d == 0:
        return [(1, 1), (-1, -1)]
    side = 1 if d > 0 else -1
    limit = size // 2 if side == far else size // 2 - 1
    return [(d + side, side)] if abs(d) < limit else []


def forwards(item):
    kind, dx, dz = item
    out = []
    if kind == "sum_x":
        return [("x", s, ("sum_x", n, 0)) for n, s in onward(dx, X, 1)]
    if kind == "sum_z":
        return [("z", s, ("sum_z", 0, n)) for n, s in onward(dz, Z, 1)]
    axis, _, far = PIECES[kind]
    if axis == "x":
        if dz == 0:
            out += [("x", s, (kind, n, 0)) for n, s in onward(dx, X, far)]
        out += [("z", s, (kind, dx, n)) for n, s in onward(dz, Z, 1 if (dx % X, kind) in UP else -1)]
    else:
        if dx == 0:
            out += [("z", s, (kind, 0, n)) for n, s in onward(dz, Z, far)]
        out += [("x", s, (kind, n, dz)) for n, s in onward(dx, X, 1 if dz % 2 == 0 else -1)]
    return out


def left_to_go(item):
    after = forwards(item)
    return 1 + max(left_to_go(n) for _, _, n in after) if after else 0


def plan():
    links = {(a, s): [] for a in "xz" for s in (1, -1)}
    given = {k: [] for k in links}
    events, tick, steps = [], itertools.count(), []
    norm_x, norm_z, waits = 1, 1, 0

    def cost(item):
        return (1024 if isinstance(item[0], str) else PIECES[item[0]][1] * 128) / RATE

    def offer(item):
        for axis, side, there in forwards(item):
            rank = -1000 if isinstance(item[0], str) else -left_to_go(there)
            links[axis, side].append((rank, next(tick), item, there))

    def begin(k, now):
        item = given[k][0]
        heapq.heappush(events, (now + cost(item), next(tick), "done", k, item))

    def feed(now):
        for k in links:
            while links[k] and len(given[k]) < DEPTH:
                links[k].sort()
                _, _, item, there = links[k].pop(0)
                steps.append(("send", k[0], k[1], item, there))
                given[k].append(there)
                if len(given[k]) == 1:
                    begin(k, now)

    for kind in FIRST:
        offer((kind, 0, 0))
    feed(0.0)
    while events:
        now, _, what, k, item = heapq.heappop(events)
        if what == "done":
            given[k].pop(0)
            if given[k]:
                begin(k, now)
            heapq.heappush(events, (now + HOP, next(tick), "here", k, item))
            feed(now)
            continue
        steps.append(("wait", item))
        waits += 1
        if waits == MEET:
            steps.append(("meet",))
            offer(("sum_x", 0, 0))
        if item[0] == "sum_x":
            norm_x += 1
            if norm_x == X:
                offer(("sum_z", 0, 0))
        elif item[0] == "sum_z":
            norm_z += 1
        offer(item)
        feed(now)
        if item[0] == "sum_z" and norm_z == Z:
            steps.append(("join",))
    return steps


def kernel(
    steps, places, tq, lq, hq, tk, lk, hk, tv, lv, hv, nt, ns, oq, ok, ov, on, *scratch
):
    vin, blocks, sums = scratch[:11], scratch[11 : 11 + len(PIECES)], scratch[11 + len(PIECES)]
    in_sem, send_sem, recv_sem, pair_sem = scratch[12 + len(PIECES) :]
    me, tp = lax.axis_index("rows"), lax.axis_index("tp")
    mz, mx = me // X, me % X

    def row(dx, dz):
        return ((mz - dz + Z) % Z) * X + (mx - dx + X) % X

    barrier = pltpu.get_barrier_semaphore()
    for there in (row(1, 0), row(-1, 0), row(0, 1), row(0, -1)):
        pl.semaphore_signal(barrier, inc=1, device_id={"rows": there}, device_id_type=MESH)

    @pl.when(tp == 0)
    def _():
        pl.semaphore_signal(barrier, inc=1, device_id={"tp": 1}, device_id_type=MESH)


    loads = [
        pltpu.make_async_copy(a, b, in_sem.at[i])
        for i, (a, b) in enumerate(zip((tq, lq, hq, tk, lk, hk, tv, lv, hv, nt, ns), vin))
    ]
    for load in loads[3:] + loads[:3]:
        load.start()
    for load in loads[3:]:
        load.wait()
    vtq, vlq, vhq, vtk, vlk, vhk, vtv, vlv, vhv, vnt, vns = vin

    def merged(train, low, high, lo, hi):
        product = lax.dot_general(
            low[...], high[:, lo:hi], (((0,), (0,)), ((), ())), preferred_element_type=jnp.float32
        )
        return (train[:, lo:hi].astype(jnp.float32) + mix_rate * product).astype(jnp.bfloat16)

    sources = ((vtq, vlq, vhq), (vtk, vlk, vhk), (vtv, vlv, vhv))
    outs = (oq, ok, ov)

    def merge(kind):
        at = 0
        for array, lo, hi in SPANS[kind]:
            blocks[kind][me, :, at : at + hi - lo] = merged(*sources[array], lo, hi)
            at += hi - lo

    def merge_query():
        for load in loads[:3]:
            load.wait()
        for kind in range(1, len(PIECES)):
            merge(kind)

    sums[me, tp] = jnp.concatenate(
        [vnt[...] + vns[...], jnp.zeros((1, 128 - vnt.shape[1]), jnp.float32)], axis=1
    )
    merge(0)
    pl.semaphore_wait(barrier, 4 + tp)

    def pair_copy(core):
        return pltpu.make_async_remote_copy(
            src_ref=sums.at[me, core],
            dst_ref=sums.at[me, core],
            send_sem=pair_sem.at[0],
            recv_sem=pair_sem.at[1],
            device_id={"tp": 1 - tp},
            device_id_type=MESH,
        )

    @pl.when(tp == 1)
    def _():
        pair_copy(1).start()

    def send_sem_of(kind):
        return send_sem.at[("sum_x", "sum_z").index(kind) + len(PIECES) if isinstance(kind, str) else kind]

    def all_sent(kind):
        count = Z * X - 1
        if kind == "sum_x":
            ref = sums.at[pl.ds(0, X - 1)]
        elif kind == "sum_z":
            ref = sums.at[pl.ds(0, (Z - 1) * X)]
        else:
            ref = blocks[kind].at[pl.ds(0, count)]
        pltpu.make_async_remote_copy(
            src_ref=ref,
            dst_ref=ref,
            send_sem=send_sem_of(kind),
            recv_sem=recv_sem.at[0],
            device_id={"rows": row(1, 0)},
            device_id_type=MESH,
        ).wait_send()

    def copy(axis, side, item, there):
        kind, dx, dz = item
        if kind == "sum_x":
            ref = sums.at[row(dx, 0)]
        elif kind == "sum_z":
            ref = sums.at[pl.ds(((mz - dz + Z) % Z) * X, X)]
        else:
            ref = blocks[kind].at[row(dx, dz)]
        target = row(-side, 0) if axis == "x" else row(0, -side)
        n = places[there]
        return pltpu.make_async_remote_copy(
            src_ref=ref,
            dst_ref=ref,
            send_sem=send_sem_of(kind),
            recv_sem=recv_sem.at[n],
            device_id={"rows": target},
            device_id_type=MESH,
        )

    def landed(item):
        kind, dx, dz = item
        if kind == "sum_x":
            ref = sums.at[row(dx, 0)]
        elif kind == "sum_z":
            ref = sums.at[pl.ds(((mz - dz + Z) % Z) * X, X)]
        else:
            ref = blocks[kind].at[row(dx, dz)]
        n = places[item]
        return pltpu.make_async_remote_copy(
            src_ref=ref,
            dst_ref=ref,
            send_sem=send_sem_of(kind),
            recv_sem=recv_sem.at[n],
            device_id={"rows": row(1, 0)},
            device_id_type=MESH,
        )

    def turn(kind, pair):
        both = blocks[kind][pl.ds(pair * 2, 2)]
        rows, columns = both.shape[1], both.shape[2]
        lanes = pl.ds(pl.multiple_of(pair * 2 * rows, 2 * rows), 2 * rows)
        flat = both.reshape(2 * rows, columns)
        at = 0
        for array, lo, hi in SPANS[kind]:
            outs[array][lo:hi, lanes] = flat[:, at : at + hi - lo].T
            at += hi - lo

    def join_norm():
        parts = sums[...].reshape(Z * X // 2, 4, 128)
        total = parts[:, 0]
        for j in range(1, 4):
            total = total + pltpu.roll(parts[:, j], 32 * j, axis=1)
        on[...] = total.astype(jnp.bfloat16)

    merged_all, later = False, []
    here = {(kind, dz): {0} if dz == 0 else set() for kind in range(len(PIECES)) for dz in range(Z)}
    for step in steps:
        if step[0] == "send":
            kind, dx, dz = step[3]
            if not (merged_all or isinstance(kind, str) or kind == 0):
                merge_query()
                merged_all = True
            copy(*step[1:]).start()
        elif step[0] == "meet":

            @pl.when(tp == 0)
            def _():
                pair_copy(1).wait_recv()
                pair_copy(0).start()

            @pl.when(tp == 1)
            def _():
                pair_copy(0).wait_recv()

        elif step[0] == "join":
            join_norm()
        else:
            for block in later:
                turn(*block)
            later = []
            item = step[1]
            landed(item).wait_recv()
            kind, dx, dz = item
            if isinstance(kind, str):
                continue
            got = here[kind, dz % Z]
            before = {0, 1, 3} <= got, len(got) == X
            got.add(dx % X)
            after = {0, 1, 3} <= got, len(got) == X
            zz = (mz - dz + Z) % Z
            if after[0] and not before[0]:
                later.append((kind, zz * 2 + mx // 2))
            if after[1] and not before[1]:
                later.append((kind, zz * 2 + 1 - mx // 2))
    for block in later:
        turn(*block)
    for kind in ("sum_x", "sum_z", *range(len(PIECES))):
        all_sent(kind)
    pair_copy(tp).wait_send()


def write_out(*refs):
    n = len(refs) // 2
    sem = refs[-1]
    copies = [pltpu.make_async_copy(refs[i], refs[n + i], sem.at[i]) for i in range(n)]
    for c in copies:
        c.start()
    for c in copies:
        c.wait()


def local(tq, lq, hq, tk, lk, hk, tv, lv, hv, nt, ns):
    steps = plan()
    places = {s[4]: i for i, s in enumerate(s for s in steps if s[0] == "send")}
    rows, wide = tq.shape
    kv = tk.shape[1]
    n = Z * X
    args = (tq, lq.T, hq, tk, lk.T, hk, tv, lv.T, hv, nt.reshape(1, -1), ns.reshape(1, -1))
    args = tuple(pltpu.with_memory_space_constraint(a, pltpu.HBM) for a in args)
    q, k, v, norm = pl.pallas_call(
        functools.partial(kernel, steps, places),
        name="gather",
        out_shape=(
            jax.ShapeDtypeStruct((wide, n * rows), jnp.bfloat16),
            jax.ShapeDtypeStruct((kv, n * rows), jnp.bfloat16),
            jax.ShapeDtypeStruct((kv, n * rows), jnp.bfloat16),
            jax.ShapeDtypeStruct((n // 2, 128), jnp.bfloat16),
        ),
        in_specs=[pl.BlockSpec(memory_space=pltpu.HBM)] * 11,
        out_specs=(pl.BlockSpec(memory_space=pltpu.VMEM),) * 4,
        scratch_shapes=[
            *(pltpu.VMEM(a.shape, a.dtype) for a in args),
            *(pltpu.VMEM((n, rows, columns), jnp.bfloat16) for _, columns, _ in PIECES),
            pltpu.VMEM((n, 2, 1, 128), jnp.float32),
            pltpu.SemaphoreType.DMA((11,)),
            pltpu.SemaphoreType.DMA((len(PIECES) + 2,)),
            pltpu.SemaphoreType.DMA((len(places),)),
            pltpu.SemaphoreType.DMA((2,)),
        ],
        compiler_params=pltpu.CompilerParams(
            collective_id=0, has_side_effects=True, vmem_limit_bytes=24 * 1024 * 1024
        ),
    )(*args)
    held = tuple(pltpu.with_memory_space_constraint(a, pltpu.VMEM) for a in (q, k, v, norm))
    q, k, v, norm = pl.pallas_call(
        write_out,
        name="write",
        out_shape=tuple(jax.ShapeDtypeStruct(a.shape, a.dtype) for a in held),
        in_specs=[pl.BlockSpec(memory_space=pltpu.VMEM)] * 4,
        out_specs=(pl.BlockSpec(memory_space=pltpu.HBM),) * 4,
        scratch_shapes=[pltpu.SemaphoreType.DMA((4,))],
        compiler_params=pltpu.CompilerParams(vmem_limit_bytes=1024 * 1024),
    )(*held)
    return q, k, v, norm.reshape(-1)


def solution(mesh):
    in_specs = (
        P(("job", "rows"), "tp"),
        P(("job", "rows"), None),
        P("job", "tp"),
        P(("job", "rows"), "tp"),
        P(("job", "rows"), None),
        P("job", "tp"),
        P(("job", "rows"), "tp"),
        P(("job", "rows"), None),
        P("job", "tp"),
        P(("job", "rows", "tp")),
        P(("job", "rows", "tp")),
    )
    out_specs = (P(("job", "tp"), None), P(("job", "tp"), None), P(("job", "tp"), None), P("job"))
    return jax.shard_map(local, mesh=mesh, in_specs=in_specs, out_specs=out_specs, check_vma=False)
```
